32 devices in a mesh: row: 8 (over z, y), expert: 4 (over x, core).
Axes of the slice: x: 2, y: 2, z: 4, core: 2. Of those that a mesh axis runs over, the one named last changes fastest.
Arguments:
- base: bfloat16 [8, 7168, 2048], P('expert', 'row'), may hold values from -6 to 6
- left_factors: bfloat16 [8, 7168, 64], P('expert', None, 'row'), may hold values from -6 to 6
- right_factors: bfloat16 [8, 64, 2048], P('expert', None, 'row'), may hold values from -0.75 to 0.75
- expert_adapter_scale: float32 [8], P('expert'), may hold values from 0.5 to 2
- placement: int32 [8], P('expert'), may hold values from 0 to 3, as said below
Outputs:
- serving: bfloat16 [8, 7168, 2048], P('expert', None, 'row')
The draws below stay inside these ranges and needn't reach their ends.
Inputs may be any that keep to these rules, and one draw needn't show every extreme that they name: `placement`: expert g * 2 + j is placed on (g + o_j) mod (4) for one offset o_j per slot j, the same for every g; the offsets of slots 0 and 1 add up to 3.
All inputs are finite; a program needn't handle non-finite values.
Results may differ from the reference program's by a relative error of at most 0.001.
Values may be sent and summed in bfloat16 or wider, within the bound.
A program may use at most 64 MiB of HBM per device.

```python
import math
import jax
import jax.numpy as jnp
from jax import lax

MODEL_WIDTH = 7168
HIDDEN_UNITS = 2048
ADAPTER_RANK = 64
EXP_DEV = 2
EXPERT_TOTAL = 8


def draw_placement(key, part):
    group_count = EXPERT_TOTAL // EXP_DEV
    offsets = jax.random.randint(jax.random.fold_in(key, 17), (EXP_DEV,), 0, group_count)
    offsets = offsets.at[1].set(group_count - 1 - offsets[0])
    expert_ids = jnp.arange(EXPERT_TOTAL, dtype=jnp.int32)
    group_ids = expert_ids // EXP_DEV
    slot_ids = expert_ids % EXP_DEV
    return jnp.mod(group_ids + offsets[slot_ids], group_count).astype(jnp.int32)


def shard_levels(rng, shape, shards, smallest, top_value):
    def one(position, parts):
        draws = jax.random.uniform(jax.random.fold_in(jax.random.fold_in(rng, 6), position), (parts,), jnp.float32, smallest / len(shards), top_value / len(shards))
        return jnp.repeat(jnp.exp(draws), shape[position] // parts).reshape((-1,) + (1,) * (len(shape) - position - 1))

    factor_of = one(*shards[0])
    for cut in shards[1:]:
        factor_of = factor_of * one(*cut)
    return factor_of


def gaussian(stream_key, dims, spread, reach, split=(), kind=jnp.bfloat16):
    drawn = spread * jax.random.normal(stream_key, dims, jnp.float32)
    if split:
        drawn = drawn * shard_levels(stream_key, dims, split, -0.22, 0.18)
    return jnp.clip(drawn, -reach, reach).astype(kind)


def setup_inputs(seed: int = 0) -> dict:
    seeds = jax.random.split(jax.random.key(seed), 6)
    return {
        "base": gaussian(seeds[0], (EXPERT_TOTAL, MODEL_WIDTH, HIDDEN_UNITS), 1.0, 6.0, ((0, 4), (1, 8))),
        "left_factors": gaussian(seeds[1], (EXPERT_TOTAL, MODEL_WIDTH, ADAPTER_RANK), 1.0, 6.0, ((0, 4), (2, 8))),
        "right_factors": gaussian(seeds[2], (EXPERT_TOTAL, ADAPTER_RANK, HIDDEN_UNITS), ADAPTER_RANK ** -0.5, 0.75, ((0, 4), (2, 8))),
        "expert_adapter_scale": jnp.clip(jnp.exp(math.log(2.0) - 1.3862944 * jax.random.uniform(seeds[3], (EXPERT_TOTAL,), jnp.float32) ** shard_levels(seeds[3], (EXPERT_TOTAL,), ((0, 4),), -0.2, 0.2)), 0.5, 2.0),
        "placement": draw_placement(jax.random.fold_in(seeds[5], 71), 0),
    }


def combine_expert_weight(expert_items):
    tile_base, factor_b, factor_a, scale_one = expert_items
    weight_update = jnp.dot(factor_b, factor_a, preferred_element_type=jnp.float32)
    return (tile_base.astype(jnp.float32) + scale_one * weight_update).astype(jnp.bfloat16)


def reference(base, left_factors, right_factors, expert_adapter_scale, placement):
    combined_weight = lax.map(combine_expert_weight, (base, left_factors, right_factors, expert_adapter_scale))
    slot_index = jnp.arange(EXPERT_TOTAL, dtype=jnp.int32) % EXP_DEV
    target = placement.astype(jnp.int32) * EXP_DEV + slot_index
    return jnp.zeros_like(combined_weight).at[target].set(combined_weight)
```

```python
import functools

import jax
import jax.numpy as jnp
from jax import lax
from jax.experimental import pallas as pl
from jax.experimental.pallas import tpu as pltpu
from jax.sharding import PartitionSpec as P

MESH = pl.DeviceIdType.MESH
WINDOW = 8
LANES = 128
VMEM_LIMIT = 24 << 20


def unit_of(height):
    return next(u for u in (1, 2, 4, 8) if u * height % LANES == 0)


def near_turn(q, half):
    quarter = half // 2
    return (q + q // quarter) % half + quarter * (1 - (q + half - 1) // half)


def piece_order(rows, unit):
    half = rows // 2
    order = []
    for q in range(half // unit):
        for m in (half + q * unit, near_turn(q, half // unit) * unit):
            order += range(m, m + unit)
    return order


def exchange_kernel(dist, groups, rows, base, left, right, scale, got, left_all, right_got, scale_got,
                    send, recv, lsend, lrecv, ssend, srecv):
    r, g = lax.axis_index("row"), lax.axis_index("expert")
    slots, _, height, width = got.shape
    to = [lax.rem(g + d, groups) for d in dist]

    barrier = pltpu.get_barrier_semaphore()
    steps = sorted({d for d in dist} | {(groups - d) % groups for d in dist} | {0})
    for e in steps:
        for m in range(rows):
            if e == 0 and m == 0:
                continue
            pl.semaphore_signal(barrier, inc=1, device_id={"row": r ^ m, "expert": lax.rem(g + e, groups)},
                                device_id_type=MESH)
    pl.semaphore_wait(barrier, len(steps) * rows - 1)

    def remote(src, dst, s, t, row, expert):
        return pltpu.make_async_remote_copy(src_ref=src, dst_ref=dst, send_sem=s, recv_sem=t,
                                            device_id={"row": row, "expert": expert}, device_id_type=MESH)

    first = []
    for j in range(slots):
        for src, dst, s, t in (
            (left.at[j], left_all.at[j, r], lsend.at[j, 0], lrecv.at[j, 0]),
            (right.at[j], right_got.at[j], ssend.at[j, 0], srecv.at[j, 0]),
            (scale.at[j], scale_got.at[j], ssend.at[j, 1], srecv.at[j, 1]),
        ):
            if dist[j] == 0:
                copy = pltpu.make_async_copy(src, dst, t)
            else:
                copy = remote(src, dst, s, t, r, to[j])
            copy.start()
            first.append(copy)

    def left_round(mask, held):
        copies = []
        for s in held:
            for j in range(slots):
                piece = left_all.at[j, r ^ s]
                copy = remote(piece, piece, lsend.at[j, mask | s], lrecv.at[j, mask | s], r ^ mask, g)
                copy.start()
                copies.append(copy)
        return copies

    rounds = []
    mask, held = rows // 2, [0]
    while mask:
        rounds.append((mask, list(held)))
        held += [s | mask for s in held]
        mask //= 2

    pieces = [(m, j) for m in piece_order(rows, unit_of(height)) for j in range(slots)]
    at = {1 + i * (len(pieces) // len(rounds)): i for i in range(len(rounds))}
    pending, waiting = [], first
    for k, (m, j) in enumerate(pieces):
        if k in at:
            for copy in waiting:
                copy.wait()
            waiting = left_round(*rounds[at[k]])
        if len(pending) >= WINDOW:
            pending.pop(0).wait_send()
        c = r ^ m
        src = base.at[j, :, pl.ds(pl.multiple_of(c * width, width), width)]
        if m == 0 and dist[j] == 0:
            pltpu.make_async_copy(src, got.at[j, r], recv.at[j, 0]).start()
        else:
            copy = remote(src, got.at[j, r], send.at[j, m], recv.at[j, m], c, to[j])
            copy.start()
            pending.append(copy)
    for copy in waiting:
        copy.wait()

    unit = unit_of(height)
    half = rows // 2
    turns = rows * slots // unit

    def place(t):
        q, f, j = t // (2 * slots), t // slots % 2, t % slots
        m = (1 - f) * (half + q * unit) + f * near_turn(q, half // unit) * unit
        return m, j, (r ^ m) // unit * unit

    def turn(t, carry):
        m, j, row = place(t)
        for u in range(unit):
            block = got.at[j, r ^ (m + u)]
            remote(block, block, send.at[j, m + u], recv.at[j, m + u], r ^ 1, g).wait_recv()
        rank_all = left_all.shape[1] * left_all.shape[2]
        columns = pl.ds(pl.multiple_of(row * height, LANES), unit * height)
        a = left_all[j, :, :, columns].reshape(rank_all, unit * height)
        delta = lax.dot_general(a, right_got[j], (((0,), (0,)), ((), ())), preferred_element_type=jnp.float32)
        weight = scale_got[j, 0:1, 0:1]
        for u in range(unit):
            part = delta[u * height:(u + 1) * height]
            got[j, row + u] = (got[j, row + u].astype(jnp.float32) + weight * part).astype(got.dtype)
        return carry

    lax.fori_loop(0, turns, turn, 0)
    for copy in pending:
        copy.wait_send()


def exchange(first, groups, rows, base, left, right, scale):
    dist = (first, groups - 1 - first)
    slots, height, total = base.shape
    width = total // rows
    rank, model = left.shape[1:]
    anywhere = pl.BlockSpec(memory_space=pl.ANY)
    dma = pltpu.SemaphoreType.DMA
    served = pl.pallas_call(
        functools.partial(exchange_kernel, dist, groups, rows),
        out_shape=jax.ShapeDtypeStruct((slots, rows, height, width), base.dtype),
        in_specs=[anywhere] * 4,
        out_specs=pl.BlockSpec(memory_space=pltpu.VMEM),
        scratch_shapes=[
            pltpu.VMEM((slots, rows, rank, model), left.dtype),
            pltpu.VMEM(right.shape, right.dtype),
            pltpu.VMEM(scale.shape, scale.dtype),
            dma((slots, rows)), dma((slots, rows)),
            dma((slots, rows)), dma((slots, rows)),
            dma((slots, 2)), dma((slots, 2)),
        ],
        compiler_params=pltpu.CompilerParams(collective_id=first, has_side_effects=True, vmem_limit_bytes=VMEM_LIMIT),
        name=f"exchange_{first}",
    )(base, left, right, scale)
    return copy_out(served.reshape(slots, rows * height, width))


def copy_out_kernel(chunks, x, y, sem):
    size = x.shape[1] // chunks
    copies = []
    for j in range(x.shape[0]):
        for i in range(chunks):
            here = pl.ds(i * size, size)
            copies.append(pltpu.make_async_copy(x.at[j, here], y.at[j, here], sem.at[j, i]))
    for copy in copies:
        copy.start()
    for copy in copies:
        copy.wait()


def copy_out(x, chunks=7):
    return pl.pallas_call(
        functools.partial(copy_out_kernel, chunks),
        out_shape=pltpu.HBM(x.shape, x.dtype),
        in_specs=[pl.BlockSpec(memory_space=pltpu.VMEM)],
        out_specs=pl.BlockSpec(memory_space=pl.ANY),
        scratch_shapes=[pltpu.SemaphoreType.DMA((x.shape[0], chunks))],
        compiler_params=pltpu.CompilerParams(vmem_limit_bytes=VMEM_LIMIT),
        name="copy_out",
    )(x)


def local(groups, rows, base, left_factors, right_factors, expert_adapter_scale, placement):
    first = jnp.mod(placement[0] - lax.axis_index("expert"), groups)
    slots = base.shape[0]
    left = jnp.swapaxes(left_factors, 1, 2)
    scale = jnp.broadcast_to(expert_adapter_scale[:, None, None], (slots, 8, 128))
    served = lax.switch(
        first,
        [functools.partial(exchange, o, groups, rows) for o in range(groups)],
        base, left, right_factors, scale,
    )
    return served


def solution(mesh):
    placed = (
        P("expert", "row", None),
        P("expert", None, "row"),
        P("expert", None, "row"),
        P("expert"),
        P("expert"),
    )
    return jax.shard_map(
        functools.partial(local, mesh.shape["expert"], mesh.shape["row"]),
        mesh=mesh, in_specs=placed, out_specs=P("expert", None, "row"), check_vma=False,
    )
```

```python
import functools

import jax
import jax.numpy as jnp
from jax import lax
from jax.experimental import pallas as pl
from jax.experimental.pallas import tpu as pltpu
from jax.sharding import PartitionSpec as P

MESH = pl.DeviceIdType.MESH
WINDOW = 12
LANES = 128
VMEM_LIMIT = 24 << 20


def unit_of(height):
    return next(u for u in (1, 2, 4, 8) if u * height % LANES == 0)


def near_turn(q, half):
    quarter = half // 2
    return (q + q // quarter) % half + quarter * (1 - (q + half - 1) // half)


def piece_order(rows, slots, lead):
    half = rows // 2
    order = []
    for q in range(half):
        for m in (half + q, near_turn(q, half)):
            order += [(m, (lead + i) % slots) for i in range(slots)]
    return order


def exchange_kernel(dist, groups, rows, base, left, right, scale, got, left_all, right_got, scale_got,
                    send, recv, tsend, trecv, lsend, lrecv, ssend, srecv, go):
    r, g = lax.axis_index("row"), lax.axis_index("expert")
    slots, _, height, width = got.shape
    half, quarter = rows // 2, rows // 4
    to = [lax.rem(g + d, groups) for d in dist]
    lead = min(range(slots), key=lambda j: min(dist[j], groups - dist[j]))
    order = piece_order(rows, slots, lead)
    mirror = half + quarter
    inner = jnp.logical_and(r >= quarter, r < rows - quarter)

    barrier = pltpu.get_barrier_semaphore()

    def enter(row, expert):
        pl.semaphore_signal(barrier, inc=1, device_id={"row": row, "expert": expert}, device_id_type=MESH)

    @pl.when(inner)
    def _():
        enter(r ^ mirror, lax.rem(g + groups - dist[lead], groups))

    steps = sorted({d for d in dist} | {(groups - d) % groups for d in dist} | {0})
    for e in steps:
        for row in (*range(quarter), *range(rows - quarter, rows)):
            if e:
                enter(row, lax.rem(g + e, groups))
            else:
                pl.when(r != row)(functools.partial(enter, row, g))
    pl.semaphore_wait(barrier, jnp.where(inner, 1, len(steps) * rows - 1))

    def remote(src, dst, s, t, row, expert):
        return pltpu.make_async_remote_copy(src_ref=src, dst_ref=dst, send_sem=s, recv_sem=t,
                                            device_id={"row": row, "expert": expert}, device_id_type=MESH)

    cuts = [(0, height)]
    if height % LANES == 0 and height > LANES:
        top = (height // LANES + 1) // 2 * LANES
        cuts = [(0, top), (top, height - top)]

    def tail(j, i):
        off, size = cuts[i]
        c = r ^ (rows - 1)
        src = base.at[j, pl.ds(off, size), pl.ds(pl.multiple_of(c * width, width), width)]
        return remote(src, got.at[j, r, pl.ds(off, size)], tsend.at[j, i], trecv.at[j, i], c, to[j])

    def piece(m, j):
        if m == rows - 1 and len(cuts) > 1:
            return [tail(j, i) for i in range(len(cuts))]
        if j == lead and m in (half, mirror):
            m = jnp.where(inner, half + mirror - m, m)
        c = r ^ m
        src = base.at[j, :, pl.ds(pl.multiple_of(c * width, width), width)]
        if dist[j] == 0 and isinstance(m, int) and m == 0:
            return [pltpu.make_async_copy(src, got.at[j, r], recv.at[j, 0])]
        return [remote(src, got.at[j, r], send.at[j, m], recv.at[j, m], c, to[j])]

    pending = piece(*order[0])

    @pl.when(inner)
    def _():
        pending[0].start()
        pl.semaphore_wait(go, 1)

    @pl.when(jnp.logical_not(inner))
    def _():
        pl.semaphore_signal(go, inc=1, device_id={"row": r ^ quarter, "expert": g}, device_id_type=MESH)

    first = []
    for j in range(slots):
        for src, dst, s, t in (
            (left.at[j], left_all.at[j, r], lsend.at[j, 0], lrecv.at[j, 0]),
            (right.at[j], right_got.at[j], ssend.at[j, 0], srecv.at[j, 0]),
            (scale, scale_got.at[j], ssend.at[j, 1], srecv.at[j, 1]),
        ):
            if dist[j] == 0:
                copy = pltpu.make_async_copy(src, dst, t)
            else:
                copy = remote(src, dst, s, t, r, to[j])
            copy.start()
            first.append(copy)
        copy = remote(left.at[j], left_all.at[j, r], lsend.at[j, half], lrecv.at[j, half], r ^ half, to[j])
        copy.start()
        first.append(copy)

    pl.when(jnp.logical_not(inner))(pending[0].start)

    def left_round(mask, held):
        copies = []
        for s in held:
            for j in range(slots):
                part = left_all.at[j, r ^ s]
                copy = remote(part, part, lsend.at[j, mask | s], lrecv.at[j, mask | s], r ^ mask, g)
                copy.start()
                copies.append(copy)
        return copies

    rounds = []
    mask, held = half // 2, [0, half]
    while mask:
        rounds.append((mask, list(held)))
        held += [s | mask for s in held]
        mask //= 2

    at = {(2 + i) * len(order) // 4: i for i in range(len(rounds))}
    waiting = first
    for k, (m, j) in enumerate(order[1:], 1):
        if k in at:
            for copy in waiting:
                copy.wait()
            waiting = left_round(*rounds[at[k]])
        if len(pending) >= WINDOW:
            pending.pop(0).wait_send()
        copies = piece(m, j)
        for copy in copies:
            copy.start()
        if not (m == 0 and dist[j] == 0):
            pending += copies
    for copy in waiting:
        copy.wait()

    unit = unit_of(height)
    rank_all = left_all.shape[1] * left_all.shape[2]

    def merge(j, row, off, size):
        columns = pl.ds(pl.multiple_of(row * height + off, LANES), size)
        a = left_all[j, :, :, columns].reshape(rank_all, size)
        return lax.dot_general(a, right_got[j], (((0,), (0,)), ((), ())), preferred_element_type=jnp.float32)

    def turn(t, carry):
        m, j = t // slots * unit, t % slots
        row = (r ^ m) // unit * unit
        for u in range(unit):
            block = got.at[j, r ^ (m + u)]
            remote(block, block, send.at[j, m + u], recv.at[j, m + u], r ^ 1, g).wait_recv()
        delta = merge(j, row, 0, unit * height)
        for u in range(unit):
            part = delta[u * height:(u + 1) * height]
            got[j, row + u] = (got[j, row + u].astype(jnp.float32) + scale_got[j, j] * part).astype(got.dtype)
        return carry

    last = 1 if len(cuts) > 1 else 0
    lax.fori_loop(0, rows * slots // unit - last * slots, turn, 0)

    row = r ^ (rows - 1)
    for j in range(slots if last else 0):
        for i, (off, size) in enumerate(cuts):
            tail(j, i).wait_recv()
            here = pl.ds(off, size)
            part = scale_got[j, j] * merge(j, row, off, size)
            got[j, row, here] = (got[j, row, here].astype(jnp.float32) + part).astype(got.dtype)
    for copy in pending:
        copy.wait_send()


def exchange(first, groups, rows, base, left, right, scale):
    dist = (first, groups - 1 - first)
    slots, height, total = base.shape
    width = total // rows
    rank, model = left.shape[1:]
    anywhere = pl.BlockSpec(memory_space=pl.ANY)
    dma = pltpu.SemaphoreType.DMA
    served = pl.pallas_call(
        functools.partial(exchange_kernel, dist, groups, rows),
        out_shape=jax.ShapeDtypeStruct((slots, rows, height, width), base.dtype),
        in_specs=[anywhere] * 4,
        out_specs=pl.BlockSpec(memory_space=pltpu.VMEM),
        scratch_shapes=[
            pltpu.VMEM((slots, rows, rank, model), left.dtype),
            pltpu.VMEM(right.shape, right.dtype),
            pltpu.SMEM((slots, slots), scale.dtype),
            dma((slots, rows)), dma((slots, rows)),
            dma((slots, 2)), dma((slots, 2)),
            dma((slots, rows)), dma((slots, rows)),
            dma((slots, 2)), dma((slots, 2)),
            pltpu.SemaphoreType.REGULAR,
        ],
        compiler_params=pltpu.CompilerParams(collective_id=first, has_side_effects=True, vmem_limit_bytes=VMEM_LIMIT),
        name=f"exchange_{first}",
    )(base, left, right, scale)
    return copy_out(served.reshape(slots, rows * height, width))


def copy_out_kernel(chunks, x, y, sem):
    size = x.shape[1] // chunks
    copies = []
    for j in range(x.shape[0]):
        for i in range(chunks):
            here = pl.ds(i * size, size)
            copies.append(pltpu.make_async_copy(x.at[j, here], y.at[j, here], sem.at[j, i]))
    for copy in copies:
        copy.start()
    for copy in copies:
        copy.wait()


def copy_out(x, chunks=7):
    return pl.pallas_call(
        functools.partial(copy_out_kernel, chunks),
        out_shape=pltpu.HBM(x.shape, x.dtype),
        in_specs=[pl.BlockSpec(memory_space=pltpu.VMEM)],
        out_specs=pl.BlockSpec(memory_space=pl.ANY),
        scratch_shapes=[pltpu.SemaphoreType.DMA((x.shape[0], chunks))],
        compiler_params=pltpu.CompilerParams(vmem_limit_bytes=VMEM_LIMIT),
        name="copy_out",
    )(x)


def local(groups, rows, base, left_factors, right_factors, expert_adapter_scale, placement):
    first = jnp.mod(placement[0] - lax.axis_index("expert"), groups)
    left = jnp.swapaxes(left_factors, 1, 2)
    served = lax.switch(
        first,
        [functools.partial(exchange, o, groups, rows) for o in range(groups)],
        base, left, right_factors, expert_adapter_scale,
    )
    return served


def solution(mesh):
    placed = (
        P("expert", "row", None),
        P("expert", None, "row"),
        P("expert", None, "row"),
        P("expert"),
        P("expert"),
    )
    return jax.shard_map(
        functools.partial(local, mesh.shape["expert"], mesh.shape["row"]),
        mesh=mesh, in_specs=placed, out_specs=P("expert", None, "row"), check_vma=False,
    )
```

```python
import functools

import jax
import jax.numpy as jnp
from jax import lax
from jax.experimental import pallas as pl
from jax.experimental.pallas import tpu as pltpu
from jax.sharding import PartitionSpec as P

MESH = pl.DeviceIdType.MESH
LANES = 128
VMEM_LIMIT = 24 << 20


def unit_of(height):
    return next(u for u in (1, 2, 4, 8) if u * height % LANES == 0)


def piece_order(rows, slots, lead):
    half, quarter = rows // 2, rows // 4
    far = [*range(half, half + quarter), *reversed(range(half + quarter, rows))]
    near = [m for pair in zip(range(quarter, half), [*range(1, quarter), 0]) for m in pair]
    turns = [(lead + i) % slots for i in range(slots)]
    order = []
    for q in range(half):
        order += [(far[q], j) for j in turns] + [(near[q], j) for j in turns]
    return order


def exchange_kernel(dist, groups, rows, base, left, right, scale, got, left_all, right_got, scale_got,
                    send, recv, tsend, trecv, lsend, lrecv, ssend, srecv, go):
    r, g = lax.axis_index("row"), lax.axis_index("expert")
    slots, _, height, width = got.shape
    half, quarter = rows // 2, rows // 4
    to = [lax.rem(g + d, groups) for d in dist]
    lead = min(range(slots), key=lambda j: min(dist[j], groups - dist[j]))
    order = piece_order(rows, slots, lead)
    mirror = half + quarter
    inner = jnp.logical_and(r >= quarter, r < rows - quarter)

    barrier = pltpu.get_barrier_semaphore()

    def enter(row, expert):
        pl.semaphore_signal(barrier, inc=1, device_id={"row": row, "expert": expert}, device_id_type=MESH)

    @pl.when(inner)
    def _():
        enter(r ^ mirror, lax.rem(g + groups - dist[lead], groups))

    steps = sorted({d for d in dist} | {(groups - d) % groups for d in dist} | {0})
    for e in steps:
        for row in (*range(quarter), *range(rows - quarter, rows)):
            if e:
                enter(row, lax.rem(g + e, groups))
            else:
                pl.when(r != row)(functools.partial(enter, row, g))
    pl.semaphore_wait(barrier, jnp.where(inner, 1, len(steps) * rows - 1))

    def remote(src, dst, s, t, row, expert):
        return pltpu.make_async_remote_copy(src_ref=src, dst_ref=dst, send_sem=s, recv_sem=t,
                                            device_id={"row": row, "expert": expert}, device_id_type=MESH)

    cuts = [(0, height)]
    if height % LANES == 0 and height > LANES:
        top = max(1, 3 * height // LANES // 4) * LANES
        cuts = [(0, top), (top, height - top)]

    def cut(i):
        if len(cuts) == 1:
            return piece(mirror, lead)
        off, size = cuts[i]
        c = r ^ mirror
        src = base.at[lead, pl.ds(off, size), pl.ds(pl.multiple_of(c * width, width), width)]
        return remote(src, got.at[lead, r, pl.ds(off, size)], tsend.at[i], trecv.at[i], c, to[lead])

    def piece(m, j):
        c = r ^ m
        src = base.at[j, :, pl.ds(pl.multiple_of(c * width, width), width)]
        if dist[j] == 0 and isinstance(m, int) and m == 0:
            return pltpu.make_async_copy(src, got.at[j, r], recv.at[j, 0])
        return remote(src, got.at[j, r], send.at[j, m], recv.at[j, m], c, to[j])

    leads = [m for m, j in order if j == lead and m >= half]

    def send_piece(m, j):
        if j != lead or m < half:
            piece(m, j).start()
            return
        q = leads.index(m)

        @pl.when(inner)
        def _():
            piece(leads[q - 1], j).start()

        @pl.when(jnp.logical_not(inner))
        def _():
            if m == mirror:
                for i in range(len(cuts)):
                    cut(i).start()
            else:
                piece(m, j).start()

    @pl.when(inner)
    def _():
        cut(0).start()
        pl.semaphore_wait(go, 1)

    @pl.when(jnp.logical_not(inner))
    def _():
        pl.semaphore_signal(go, inc=1, device_id={"row": r ^ quarter, "expert": g}, device_id_type=MESH)

    first = []
    for j in range(slots):
        for src, dst, s, t in (
            (left.at[j], left_all.at[j, r], lsend.at[j, 0], lrecv.at[j, 0]),
            (right.at[j], right_got.at[j], ssend.at[j, 0], srecv.at[j, 0]),
            (scale, scale_got.at[j], ssend.at[j, 1], srecv.at[j, 1]),
        ):
            if dist[j] == 0:
                copy = pltpu.make_async_copy(src, dst, t)
            else:
                copy = remote(src, dst, s, t, r, to[j])
            copy.start()
            first.append(copy)
        copy = remote(left.at[j], left_all.at[j, r], lsend.at[j, half], lrecv.at[j, half], r ^ half, to[j])
        copy.start()
        first.append(copy)

    pl.when(jnp.logical_not(inner))(piece(*order[0]).start)

    def left_round(mask, held):
        copies = []
        for s in held:
            for j in range(slots):
                part = left_all.at[j, r ^ s]
                copy = remote(part, part, lsend.at[j, mask | s], lrecv.at[j, mask | s], r ^ mask, g)
                copy.start()
                copies.append(copy)
        return copies

    rounds = []
    mask, held = half // 2, [0, half]
    while mask:
        rounds.append((mask, list(held)))
        held += [s | mask for s in held]
        mask //= 2

    at = {(2 + i) * len(order) // 4: i for i in range(len(rounds))}
    waiting = first
    for k, (m, j) in enumerate(order[1:], 1):
        if k in at:
            for copy in waiting:
                copy.wait()
            waiting = left_round(*rounds[at[k]])
        send_piece(m, j)
    for i in range(1, len(cuts)):
        pl.when(inner)(cut(i).start)
    for copy in waiting:
        copy.wait()

    unit = unit_of(height)
    rank_all = left_all.shape[1] * left_all.shape[2]

    def merge(j, row, off, size):
        columns = pl.ds(pl.multiple_of(row * height + off, LANES), size)
        a = left_all[j, :, :, columns].reshape(rank_all, size)
        return lax.dot_general(a, right_got[j], (((0,), (0,)), ((), ())), preferred_element_type=jnp.float32)

    blocks = rows // unit
    calm = blocks - blocks // 4

    def turn(t, carry):
        q, j = t // slots, lax.rem(lead + 1 + t, slots)
        m = jnp.where(q < calm, q, calm + blocks - 1 - q) * unit
        row = (r ^ m) // unit * unit
        for u in range(unit):
            block = got.at[j, r ^ (m + u)]
            remote(block, block, send.at[j, m + u], recv.at[j, m + u], r ^ 1, g).wait_recv()
        delta = merge(j, row, 0, unit * height)
        for u in range(unit):
            part = delta[u * height:(u + 1) * height]
            got[j, row + u] = (got[j, row + u].astype(jnp.float32) + scale_got[j, j] * part).astype(got.dtype)
        return carry

    lax.fori_loop(0, blocks * slots - (len(cuts) > 1), turn, 0)
    row = r ^ mirror
    for i, (off, size) in enumerate(cuts if len(cuts) > 1 else ()):
        cut(i).wait_recv()
        here = pl.ds(off, size)
        part = scale_got[lead, lead] * merge(lead, row, off, size)
        got[lead, row, here] = (got[lead, row, here].astype(jnp.float32) + part).astype(got.dtype)
    for m, j in order:
        if (m, j) == (mirror, lead):
            for i in range(len(cuts)):
                cut(i).wait_send()
        elif m or dist[j]:
            piece(m, j).wait_send()


def exchange(first, groups, rows, base, left, right, scale):
    dist = (first, groups - 1 - first)
    slots, height, total = base.shape
    width = total // rows
    rank, model = left.shape[1:]
    anywhere = pl.BlockSpec(memory_space=pl.ANY)
    dma = pltpu.SemaphoreType.DMA
    served = pl.pallas_call(
        functools.partial(exchange_kernel, dist, groups, rows),
        out_shape=jax.ShapeDtypeStruct((slots, rows, height, width), base.dtype),
        in_specs=[anywhere] * 4,
        out_specs=pl.BlockSpec(memory_space=pltpu.VMEM),
        scratch_shapes=[
            pltpu.VMEM((slots, rows, rank, model), left.dtype),
            pltpu.VMEM(right.shape, right.dtype),
            pltpu.SMEM((slots, slots), scale.dtype),
            dma((slots, rows)), dma((slots, rows)),
            dma((2,)), dma((2,)),
            dma((slots, rows)), dma((slots, rows)),
            dma((slots, 2)), dma((slots, 2)),
            pltpu.SemaphoreType.REGULAR,
        ],
        compiler_params=pltpu.CompilerParams(collective_id=first, has_side_effects=True, vmem_limit_bytes=VMEM_LIMIT),
        name=f"exchange_{first}",
    )(base, left, right, scale)
    return copy_out(served.reshape(slots, rows * height, width))


def copy_out_kernel(chunks, x, y, sem):
    size = x.shape[1] // chunks
    copies = []
    for j in range(x.shape[0]):
        for i in range(chunks):
            here = pl.ds(i * size, size)
            copies.append(pltpu.make_async_copy(x.at[j, here], y.at[j, here], sem.at[j, i]))
    for copy in copies:
        copy.start()
    for copy in copies:
        copy.wait()


def copy_out(x, chunks=7):
    return pl.pallas_call(
        functools.partial(copy_out_kernel, chunks),
        out_shape=pltpu.HBM(x.shape, x.dtype),
        in_specs=[pl.BlockSpec(memory_space=pltpu.VMEM)],
        out_specs=pl.BlockSpec(memory_space=pl.ANY),
        scratch_shapes=[pltpu.SemaphoreType.DMA((x.shape[0], chunks))],
        compiler_params=pltpu.CompilerParams(vmem_limit_bytes=VMEM_LIMIT),
        name="copy_out",
    )(x)


def local(groups, rows, base, left_factors, right_factors, expert_adapter_scale, placement):
    first = jnp.mod(placement[0] - lax.axis_index("expert"), groups)
    left = jnp.swapaxes(left_factors, 1, 2)
    served = lax.switch(
        first,
        [functools.partial(exchange, o, groups, rows) for o in range(groups)],
        base, left, right_factors, expert_adapter_scale,
    )
    return served


def solution(mesh):
    placed = (
        P("expert", "row", None),
        P("expert", None, "row"),
        P("expert", None, "row"),
        P("expert"),
        P("expert"),
    )
    return jax.shard_map(
        functools.partial(local, mesh.shape["expert"], mesh.shape["row"]),
        mesh=mesh, in_specs=placed, out_specs=P("expert", None, "row"), check_vma=False,
    )
```

```python
import functools

import jax
import jax.numpy as jnp
from jax import lax
from jax.experimental import pallas as pl
from jax.experimental.pallas import tpu as pltpu
from jax.sharding import PartitionSpec as P

MESH = pl.DeviceIdType.MESH
LANES = 128
VMEM_LIMIT = 24 << 20


def unit_of(height):
    return next(u for u in (1, 2, 4, 8) if u * height % LANES == 0)


def piece_order(rows):
    half, quarter = rows // 2, rows // 4
    far = [*range(half, half + quarter), *reversed(range(half + quarter, rows))]
    near = [m for pair in zip(range(quarter, half), [*range(1, quarter), 0]) for m in pair]
    return [m for pair in zip(far, near) for m in pair]


def exchange_kernel(dist, groups, rows, base, left, right, scale, got, left_all, right_got, scale_got,
                    held, left_own, right_all, scale_own,
                    send, recv, tsend, trecv, lsend, lrecv, ssend, srecv, go,
                    asend, arecv, rsend, rrecv, near):
    r, g = lax.axis_index("row"), lax.axis_index("expert")
    slots, _, height, width = got.shape
    half, quarter = rows // 2, rows // 4
    to = [lax.rem(g + d, groups) for d in dist]
    lead = min(range(slots), key=lambda j: min(dist[j], groups - dist[j]))
    other = 1 - lead
    order = piece_order(rows)
    mirror = half + quarter
    inner = jnp.logical_and(r >= quarter, r < rows - quarter)

    barrier = pltpu.get_barrier_semaphore()

    def enter(row, expert):
        pl.semaphore_signal(barrier, inc=1, device_id={"row": row, "expert": expert}, device_id_type=MESH)

    @pl.when(inner)
    def _():
        enter(r ^ mirror, lax.rem(g + groups - dist[lead], groups))

    steps = sorted({d for d in dist} | {(groups - d) % groups for d in dist} | {0})
    for e in steps:
        for row in (*range(quarter), *range(rows - quarter, rows)):
            if e:
                enter(row, lax.rem(g + e, groups))
            else:
                pl.when(r != row)(functools.partial(enter, row, g))
    pl.semaphore_wait(barrier, jnp.where(inner, 1, len(steps) * rows - 1))

    def remote(src, dst, s, t, row, expert):
        return pltpu.make_async_remote_copy(src_ref=src, dst_ref=dst, send_sem=s, recv_sem=t,
                                            device_id={"row": row, "expert": expert}, device_id_type=MESH)

    cuts = [(0, height)]
    if height % LANES == 0 and height > LANES:
        top = max(1, 3 * height // LANES // 4) * LANES
        cuts = [(0, top), (top, height - top)]

    def cut(i):
        if len(cuts) == 1:
            return piece(mirror, lead)
        off, size = cuts[i]
        c = r ^ mirror
        src = base.at[lead, pl.ds(off, size), pl.ds(pl.multiple_of(c * width, width), width)]
        return remote(src, got.at[lead, r, pl.ds(off, size)], tsend.at[i], trecv.at[i], c, to[lead])

    def piece(m, j):
        c = r ^ m
        columns = pl.ds(pl.multiple_of(c * width, width), width)
        src = base.at[j, :, columns] if j == lead else held.at[:, columns]
        if dist[j] == 0 and isinstance(m, int) and m == 0:
            return pltpu.make_async_copy(src, got.at[j, r], recv.at[j, 0])
        return remote(src, got.at[j, r], send.at[j, m], recv.at[j, m], c, to[j])

    leads = [m for m in order if m >= half]

    def send_lead(m):
        if m < half:
            piece(m, lead).start()
            return
        q = leads.index(m)

        @pl.when(inner)
        def _():
            piece(leads[q - 1], lead).start()

        @pl.when(jnp.logical_not(inner))
        def _():
            if m == mirror:
                for i in range(len(cuts)):
                    cut(i).start()
            else:
                piece(m, lead).start()

    unit = unit_of(height)
    span = unit * height
    loads = [
        pltpu.make_async_copy(base.at[other], held, near.at[0]),
        pltpu.make_async_copy(right.at[other], right_all.at[r], near.at[1]),
        pltpu.make_async_copy(left.at[other, :, pl.ds(pl.multiple_of(r // unit * span, LANES), span)],
                              left_own.at[r], near.at[2]),
        pltpu.make_async_copy(scale, scale_own, near.at[3]),
    ]
    for copy in loads:
        copy.start()

    @pl.when(inner)
    def _():
        cut(0).start()
        pl.semaphore_wait(go, 1)

    @pl.when(jnp.logical_not(inner))
    def _():
        pl.semaphore_signal(go, inc=1, device_id={"row": r ^ quarter, "expert": g}, device_id_type=MESH)

    first = []
    for src, dst, s, t in (
        (left.at[lead], left_all.at[r], lsend.at[0], lrecv.at[0]),
        (right.at[lead], right_got, ssend.at[0], srecv.at[0]),
        (scale, scale_got, ssend.at[1], srecv.at[1]),
    ):
        if dist[lead] == 0:
            copy = pltpu.make_async_copy(src, dst, t)
        else:
            copy = remote(src, dst, s, t, r, to[lead])
        first.append(copy)
    first.append(remote(left.at[lead], left_all.at[r], lsend.at[half], lrecv.at[half], r ^ half, to[lead]))
    for m in (*range(half, rows), *range(1, half)):
        c = r ^ m
        part = left.at[other, :, pl.ds(pl.multiple_of(c // unit * span, LANES), span)]
        first.append(remote(part, left_own.at[r], asend.at[m], arecv.at[m], c, g))
    for m in (half, *range(1, half)):
        first.append(remote(right.at[other], right_all.at[r], rsend.at[0, m], rrecv.at[0, m], r ^ m, g))
    for copy in first:
        copy.start()

    pl.when(jnp.logical_not(inner))(piece(order[0], lead).start)

    def right_round():
        part = right_all.at[r ^ half]
        copies = [remote(part, part, rsend.at[1, m], rrecv.at[1, m], r ^ m, g) for m in range(1, half)]
        for copy in copies:
            copy.start()
        return copies

    def left_round(mask, have):
        copies = []
        for s in have:
            part = left_all.at[r ^ s]
            copy = remote(part, part, lsend.at[mask | s], lrecv.at[mask | s], r ^ mask, g)
            copy.start()
            copies.append(copy)
        return copies

    rounds = []
    mask, have = half // 2, [0, half]
    while mask:
        rounds.append((mask, list(have)))
        have += [s | mask for s in have]
        mask //= 2

    early = len(order) if dist[lead] == 0 else len(order) // 4
    for m in order[1:early]:
        send_lead(m)
    ahead = [first[3], first[3 + rows]]
    first[0].wait()
    for copy in ahead:
        copy.wait_recv()
    waiting = right_round() + left_round(*rounds[0])
    for m in order[early:]:
        send_lead(m)
    for copy in ahead:
        copy.wait_send()
    for copy in first[1:3] + first[4:3 + rows] + first[4 + rows:] + waiting + loads:
        copy.wait()
    waiting = left_round(*rounds[1])

    def expand(lhs, rhs):
        return lax.dot_general(lhs, rhs, (((0,), (0,)), ((), ())), preferred_element_type=jnp.float32)

    rank_all = left_all.shape[0] * left_all.shape[1]

    def merge_held(q, carry):
        c = r ^ q ^ half
        delta = expand(left_own[...].reshape(rank_all, span), right_all[c])
        part = delta[:height]
        for u in range(1, unit):
            part = jnp.where(lax.rem(r, unit) == u, delta[u * height:(u + 1) * height], part)
        here = pl.ds(pl.multiple_of(c * width, width), width)
        held[:, here] = (held[:, here].astype(jnp.float32) + scale_own[other] * part).astype(held.dtype)
        return carry

    lax.fori_loop(0, rows, merge_held, 0)
    for m in order:
        piece(m, other).start()
    for i in range(1, len(cuts)):
        pl.when(inner)(cut(i).start)
    for copy in waiting:
        copy.wait()
    for i in range(2, len(rounds)):
        for copy in left_round(*rounds[i]):
            copy.wait()

    def merge(row, off, size):
        columns = pl.ds(pl.multiple_of(row * height + off, LANES), size)
        return expand(left_all[:, :, columns].reshape(rank_all, size), right_got[...])

    blocks = rows // unit
    calm = blocks - blocks // 4

    def turn(q, carry):
        m = jnp.where(q < calm, q, calm + blocks - 1 - q) * unit
        row = (r ^ m) // unit * unit
        for u in range(unit):
            block = got.at[lead, r ^ (m + u)]
            remote(block, block, send.at[lead, m + u], recv.at[lead, m + u], r ^ 1, g).wait_recv()
        delta = merge(row, 0, span)
        for u in range(unit):
            part = delta[u * height:(u + 1) * height]
            got[lead, row + u] = (got[lead, row + u].astype(jnp.float32) + scale_got[lead] * part).astype(got.dtype)
        return carry

    lax.fori_loop(0, blocks - (len(cuts) > 1), turn, 0)
    for m in order:
        piece(m, other).wait_recv()
    row = r ^ mirror
    for i, (off, size) in enumerate(cuts if len(cuts) > 1 else ()):
        cut(i).wait_recv()
        here = pl.ds(off, size)
        part = scale_got[lead] * merge(row, off, size)
        got[lead, row, here] = (got[lead, row, here].astype(jnp.float32) + part).astype(got.dtype)
    for m in order:
        piece(m, other).wait_send()
        if m == mirror:
            for i in range(len(cuts)):
                cut(i).wait_send()
        elif m or dist[lead]:
            piece(m, lead).wait_send()


def exchange(first, groups, rows, base, left, right, scale):
    dist = (first, groups - 1 - first)
    slots, height, total = base.shape
    width = total // rows
    rank, model = left.shape[1:]
    anywhere = pl.BlockSpec(memory_space=pl.ANY)
    dma = pltpu.SemaphoreType.DMA
    served = pl.pallas_call(
        functools.partial(exchange_kernel, dist, groups, rows),
        out_shape=jax.ShapeDtypeStruct((slots, rows, height, width), base.dtype),
        in_specs=[anywhere] * 4,
        out_specs=pl.BlockSpec(memory_space=pltpu.VMEM),
        scratch_shapes=[
            pltpu.VMEM((rows, rank, model), left.dtype),
            pltpu.VMEM(right.shape[1:], right.dtype),
            pltpu.SMEM(scale.shape, scale.dtype),
            pltpu.VMEM((height, total), base.dtype),
            pltpu.VMEM((rows, rank, unit_of(height) * height), left.dtype),
            pltpu.VMEM((rows, *right.shape[1:]), right.dtype),
            pltpu.SMEM(scale.shape, scale.dtype),
            dma((slots, rows)), dma((slots, rows)),
            dma((2,)), dma((2,)),
            dma((rows,)), dma((rows,)),
            dma((2,)), dma((2,)),
            pltpu.SemaphoreType.REGULAR,
            dma((rows,)), dma((rows,)),
            dma((2, rows)), dma((2, rows)),
            dma((4,)),
        ],
        compiler_params=pltpu.CompilerParams(collective_id=first, has_side_effects=True, vmem_limit_bytes=VMEM_LIMIT),
        name=f"exchange_{first}",
    )(base, left, right, scale)
    return copy_out(served.reshape(slots, rows * height, width))


def copy_out_kernel(chunks, x, y, sem):
    size = x.shape[1] // chunks
    copies = []
    for j in range(x.shape[0]):
        for i in range(chunks):
            here = pl.ds(i * size, size)
            copies.append(pltpu.make_async_copy(x.at[j, here], y.at[j, here], sem.at[j, i]))
    for copy in copies:
        copy.start()
    for copy in copies:
        copy.wait()


def copy_out(x, chunks=7):
    return pl.pallas_call(
        functools.partial(copy_out_kernel, chunks),
        out_shape=pltpu.HBM(x.shape, x.dtype),
        in_specs=[pl.BlockSpec(memory_space=pltpu.VMEM)],
        out_specs=pl.BlockSpec(memory_space=pl.ANY),
        scratch_shapes=[pltpu.SemaphoreType.DMA((x.shape[0], chunks))],
        compiler_params=pltpu.CompilerParams(vmem_limit_bytes=VMEM_LIMIT),
        name="copy_out",
    )(x)


def local(groups, rows, base, left_factors, right_factors, expert_adapter_scale, placement):
    first = jnp.mod(placement[0] - lax.axis_index("expert"), groups)
    left = jnp.swapaxes(left_factors, 1, 2)
    served = lax.switch(
        first,
        [functools.partial(exchange, o, groups, rows) for o in range(groups)],
        base, left, right_factors, expert_adapter_scale,
    )
    return served


def solution(mesh):
    placed = (
        P("expert", "row", None),
        P("expert", None, "row"),
        P("expert", None, "row"),
        P("expert"),
        P("expert"),
    )
    return jax.shard_map(
        functools.partial(local, mesh.shape["expert"], mesh.shape["row"]),
        mesh=mesh, in_specs=placed, out_specs=P("expert", None, "row"), check_vma=False,
    )
```

```python
import functools

import jax
import jax.numpy as jnp
from jax import lax
from jax.experimental import pallas as pl
from jax.experimental.pallas import tpu as pltpu
from jax.sharding import PartitionSpec as P

MESH = pl.DeviceIdType.MESH
LANES = 128
VMEM_LIMIT = 24 << 20


def unit_of(height):
    return next(u for u in (1, 2, 4, 8) if u * height % LANES == 0)


def piece_order(rows):
    half, quarter = rows // 2, rows // 4
    far = [*range(half, half + quarter), *reversed(range(half + quarter, rows))]
    near = [m for pair in zip(range(quarter, half), [*range(1, quarter), 0]) for m in pair]
    return [m for pair in zip(far, near) for m in pair]


def exchange_kernel(dist, groups, rows, base, left, right, scale, got, left_all, right_got, scale_got,
                    held, left_own, right_all, scale_own,
                    send, recv, tsend, trecv, lsend, lrecv, ssend, srecv, go,
                    asend, arecv, rsend, rrecv, near):
    r, g = lax.axis_index("row"), lax.axis_index("expert")
    slots, _, height, width = got.shape
    half, quarter = rows // 2, rows // 4
    to = [lax.rem(g + d, groups) for d in dist]
    lead = min(range(slots), key=lambda j: min(dist[j], groups - dist[j]))
    other = 1 - lead
    order = piece_order(rows)
    mirror = half + quarter
    inner = jnp.logical_and(r >= quarter, r < rows - quarter)

    barrier = pltpu.get_barrier_semaphore()

    def enter(row, expert):
        pl.semaphore_signal(barrier, inc=1, device_id={"row": row, "expert": expert}, device_id_type=MESH)

    @pl.when(inner)
    def _():
        enter(r ^ mirror, lax.rem(g + groups - dist[lead], groups))

    steps = sorted({d for d in dist} | {(groups - d) % groups for d in dist} | {0})
    for e in steps:
        for row in (*range(quarter), *range(rows - quarter, rows)):
            if e:
                enter(row, lax.rem(g + e, groups))
            else:
                pl.when(r != row)(functools.partial(enter, row, g))
    pl.semaphore_wait(barrier, jnp.where(inner, 1, len(steps) * rows - 1))

    def remote(src, dst, s, t, row, expert):
        return pltpu.make_async_remote_copy(src_ref=src, dst_ref=dst, send_sem=s, recv_sem=t,
                                            device_id={"row": row, "expert": expert}, device_id_type=MESH)

    cuts = [(0, height)]
    if height % LANES == 0 and height > LANES:
        top = max(1, 3 * height // LANES // 4) * LANES
        cuts = [(0, top), (top, height - top)]

    def cut(i):
        if len(cuts) == 1:
            return piece(mirror, lead)
        off, size = cuts[i]
        c = r ^ mirror
        src = base.at[lead, pl.ds(off, size), pl.ds(pl.multiple_of(c * width, width), width)]
        return remote(src, got.at[lead, r, pl.ds(off, size)], tsend.at[i], trecv.at[i], c, to[lead])

    def piece(m, j):
        c = r ^ m
        columns = pl.ds(pl.multiple_of(c * width, width), width)
        src = base.at[j, :, columns] if j == lead else held.at[:, columns]
        if dist[j] == 0 and isinstance(m, int) and m == 0:
            return pltpu.make_async_copy(src, got.at[j, r], recv.at[j, 0])
        return remote(src, got.at[j, r], send.at[j, m], recv.at[j, m], c, to[j])

    leads = [m for m in order if m >= half]

    def send_lead(m):
        if m < half:
            piece(m, lead).start()
            return
        q = leads.index(m)

        @pl.when(inner)
        def _():
            piece(leads[q - 1], lead).start()

        @pl.when(jnp.logical_not(inner))
        def _():
            if m == mirror:
                for i in range(len(cuts)):
                    cut(i).start()
            else:
                piece(m, lead).start()

    unit = unit_of(height)
    span = unit * height
    loads = [
        pltpu.make_async_copy(base.at[other], held, near.at[0]),
        pltpu.make_async_copy(right.at[other], right_all.at[r], near.at[1]),
        pltpu.make_async_copy(left.at[other, :, pl.ds(pl.multiple_of(r // unit * span, LANES), span)],
                              left_own.at[r], near.at[2]),
        pltpu.make_async_copy(scale, scale_own, near.at[3]),
    ]
    for copy in loads:
        copy.start()

    @pl.when(inner)
    def _():
        cut(0).start()
        pl.semaphore_wait(go, 1)

    @pl.when(jnp.logical_not(inner))
    def _():
        pl.semaphore_signal(go, inc=1, device_id={"row": r ^ quarter, "expert": g}, device_id_type=MESH)

    first = []
    for src, dst, s, t in (
        (left.at[lead], left_all.at[r], lsend.at[0], lrecv.at[0]),
        (right.at[lead], right_got, ssend.at[0], srecv.at[0]),
        (scale, scale_got, ssend.at[1], srecv.at[1]),
    ):
        if dist[lead] == 0:
            copy = pltpu.make_async_copy(src, dst, t)
        else:
            copy = remote(src, dst, s, t, r, to[lead])
        first.append(copy)
    first.append(remote(left.at[lead], left_all.at[r], lsend.at[half], lrecv.at[half], r ^ half, to[lead]))
    for m in (*range(half, rows), *range(1, half)):
        c = r ^ m
        part = left.at[other, :, pl.ds(pl.multiple_of(c // unit * span, LANES), span)]
        first.append(remote(part, left_own.at[r], asend.at[m], arecv.at[m], c, g))
    for m in (half, *range(1, half)):
        first.append(remote(right.at[other], right_all.at[r], rsend.at[0, m], rrecv.at[0, m], r ^ m, g))
    for copy in first:
        copy.start()

    pl.when(jnp.logical_not(inner))(piece(order[0], lead).start)

    def right_round():
        part = right_all.at[r ^ half]
        copies = [remote(part, part, rsend.at[1, m], rrecv.at[1, m], r ^ m, g) for m in range(1, half)]
        for copy in copies:
            copy.start()
        return copies

    def left_round(mask, have):
        copies = []
        for s in have:
            part = left_all.at[r ^ s]
            copy = remote(part, part, lsend.at[mask | s], lrecv.at[mask | s], r ^ mask, g)
            copy.start()
            copies.append(copy)
        return copies

    rounds = []
    mask, have = half // 2, [0, half]
    while mask:
        rounds.append((mask, list(have)))
        have += [s | mask for s in have]
        mask //= 2

    early = len(order) if dist[lead] == 0 else len(order) // 4
    for m in order[1:early]:
        send_lead(m)
    ahead = [first[3], first[3 + rows]]
    first[0].wait()
    for copy in ahead:
        copy.wait_recv()
    waiting = right_round() + left_round(*rounds[0])
    for m in order[early:]:
        send_lead(m)
    for copy in ahead:
        copy.wait_send()
    for copy in first[1:3] + first[4:3 + rows] + first[4 + rows:] + waiting + loads:
        copy.wait()
    waiting = left_round(*rounds[1])

    def expand(lhs, rhs):
        return lax.dot_general(lhs, rhs, (((0,), (0,)), ((), ())), preferred_element_type=jnp.float32)

    rank_all = left_all.shape[0] * left_all.shape[1]

    def merge_held(q, carry):
        c = r ^ q ^ half
        delta = expand(left_own[...].reshape(rank_all, span), right_all[c])
        part = delta[:height]
        for u in range(1, unit):
            part = jnp.where(lax.rem(r, unit) == u, delta[u * height:(u + 1) * height], part)
        here = pl.ds(pl.multiple_of(c * width, width), width)
        held[:, here] = (held[:, here].astype(jnp.float32) + scale_own[other] * part).astype(held.dtype)
        return carry

    lax.fori_loop(0, rows, merge_held, 0)
    for m in order[::2] + order[1::2] if dist[lead] == 0 else order:
        piece(m, other).start()
    for i in range(1, len(cuts)):
        pl.when(inner)(cut(i).start)
    for copy in waiting:
        copy.wait()
    for i in range(2, len(rounds)):
        for copy in left_round(*rounds[i]):
            copy.wait()

    def merge(row, off, size):
        columns = pl.ds(pl.multiple_of(row * height + off, LANES), size)
        return expand(left_all[:, :, columns].reshape(rank_all, size), right_got[...])

    blocks = rows // unit
    calm = blocks - blocks // 4

    def turn(q, carry):
        m = jnp.where(q < calm, q, calm + blocks - 1 - q) * unit
        row = (r ^ m) // unit * unit
        for u in range(unit):
            block = got.at[lead, r ^ (m + u)]
            remote(block, block, send.at[lead, m + u], recv.at[lead, m + u], r ^ 1, g).wait_recv()
        delta = merge(row, 0, span)
        for u in range(unit):
            part = delta[u * height:(u + 1) * height]
            got[lead, row + u] = (got[lead, row + u].astype(jnp.float32) + scale_got[lead] * part).astype(got.dtype)
        return carry

    lax.fori_loop(0, blocks - (len(cuts) > 1), turn, 0)
    for m in order:
        piece(m, other).wait_recv()
    row = r ^ mirror
    for i, (off, size) in enumerate(cuts if len(cuts) > 1 else ()):
        cut(i).wait_recv()
        here = pl.ds(off, size)
        part = scale_got[lead] * merge(row, off, size)
        got[lead, row, here] = (got[lead, row, here].astype(jnp.float32) + part).astype(got.dtype)
    for m in order:
        piece(m, other).wait_send()
        if m == mirror:
            for i in range(len(cuts)):
                cut(i).wait_send()
        elif m or dist[lead]:
            piece(m, lead).wait_send()


def exchange(first, groups, rows, base, left, right, scale):
    dist = (first, groups - 1 - first)
    slots, height, total = base.shape
    width = total // rows
    rank, model = left.shape[1:]
    anywhere = pl.BlockSpec(memory_space=pl.ANY)
    dma = pltpu.SemaphoreType.DMA
    served = pl.pallas_call(
        functools.partial(exchange_kernel, dist, groups, rows),
        out_shape=jax.ShapeDtypeStruct((slots, rows, height, width), base.dtype),
        in_specs=[anywhere] * 4,
        out_specs=pl.BlockSpec(memory_space=pltpu.VMEM),
        scratch_shapes=[
            pltpu.VMEM((rows, rank, model), left.dtype),
            pltpu.VMEM(right.shape[1:], right.dtype),
            pltpu.SMEM(scale.shape, scale.dtype),
            pltpu.VMEM((height, total), base.dtype),
            pltpu.VMEM((rows, rank, unit_of(height) * height), left.dtype),
            pltpu.VMEM((rows, *right.shape[1:]), right.dtype),
            pltpu.SMEM(scale.shape, scale.dtype),
            dma((slots, rows)), dma((slots, rows)),
            dma((2,)), dma((2,)),
            dma((rows,)), dma((rows,)),
            dma((2,)), dma((2,)),
            pltpu.SemaphoreType.REGULAR,
            dma((rows,)), dma((rows,)),
            dma((2, rows)), dma((2, rows)),
            dma((4,)),
        ],
        compiler_params=pltpu.CompilerParams(collective_id=first, has_side_effects=True, vmem_limit_bytes=VMEM_LIMIT),
        name=f"exchange_{first}",
    )(base, left, right, scale)
    return copy_out(served.reshape(slots, rows * height, width))


def copy_out_kernel(chunks, x, y, sem):
    size = x.shape[1] // chunks
    copies = []
    for j in range(x.shape[0]):
        for i in range(chunks):
            here = pl.ds(i * size, size)
            copies.append(pltpu.make_async_copy(x.at[j, here], y.at[j, here], sem.at[j, i]))
    for copy in copies:
        copy.start()
    for copy in copies:
        copy.wait()


def copy_out(x, chunks=7):
    return pl.pallas_call(
        functools.partial(copy_out_kernel, chunks),
        out_shape=pltpu.HBM(x.shape, x.dtype),
        in_specs=[pl.BlockSpec(memory_space=pltpu.VMEM)],
        out_specs=pl.BlockSpec(memory_space=pl.ANY),
        scratch_shapes=[pltpu.SemaphoreType.DMA((x.shape[0], chunks))],
        compiler_params=pltpu.CompilerParams(vmem_limit_bytes=VMEM_LIMIT),
        name="copy_out",
    )(x)


def local(groups, rows, base, left_factors, right_factors, expert_adapter_scale, placement):
    first = jnp.mod(placement[0] - lax.axis_index("expert"), groups)
    left = jnp.swapaxes(left_factors, 1, 2)
    served = lax.switch(
        first,
        [functools.partial(exchange, o, groups, rows) for o in range(groups)],
        base, left, right_factors, expert_adapter_scale,
    )
    return served


def solution(mesh):
    placed = (
        P("expert", "row", None),
        P("expert", None, "row"),
        P("expert", None, "row"),
        P("expert"),
        P("expert"),
    )
    return jax.shard_map(
        functools.partial(local, mesh.shape["expert"], mesh.shape["row"]),
        mesh=mesh, in_specs=placed, out_specs=P("expert", None, "row"), check_vma=False,
    )
```

```python
import functools

import jax
import jax.numpy as jnp
from jax import lax
from jax.experimental import pallas as pl
from jax.experimental.pallas import tpu as pltpu
from jax.sharding import PartitionSpec as P

MESH = pl.DeviceIdType.MESH
LANES = 128
VMEM_LIMIT = 24 << 20


def unit_of(height):
    return next(u for u in (1, 2, 4, 8) if u * height % LANES == 0)


def piece_order(rows):
    half, quarter = rows // 2, rows // 4
    far = [*range(half, half + quarter), *reversed(range(half + quarter, rows))]
    near = [m for pair in zip(range(quarter, half), [*range(1, quarter), 0]) for m in pair]
    return [m for pair in zip(far, near) for m in pair]


def exchange_kernel(dist, groups, rows, base, left, right, scale, got, left_all, right_got, scale_got,
                    held, left_own, right_all, scale_own,
                    send, recv, tsend, trecv, lsend, lrecv, ssend, srecv, go,
                    asend, arecv, rsend, rrecv, near):
    r, g = lax.axis_index("row"), lax.axis_index("expert")
    slots, _, height, width = got.shape
    half, quarter = rows // 2, rows // 4
    to = [lax.rem(g + d, groups) for d in dist]
    lead = min(range(slots), key=lambda j: min(dist[j], groups - dist[j]))
    other = 1 - lead
    order = piece_order(rows)
    mirror = half + quarter
    inner = jnp.logical_and(r >= quarter, r < rows - quarter)

    barrier = pltpu.get_barrier_semaphore()

    def enter(row, expert):
        pl.semaphore_signal(barrier, inc=1, device_id={"row": row, "expert": expert}, device_id_type=MESH)

    @pl.when(inner)
    def _():
        enter(r ^ mirror, lax.rem(g + groups - dist[lead], groups))

    steps = sorted({d for d in dist} | {(groups - d) % groups for d in dist} | {0})
    for e in steps:
        for row in (*range(quarter), *range(rows - quarter, rows)):
            if e:
                enter(row, lax.rem(g + e, groups))
            else:
                pl.when(r != row)(functools.partial(enter, row, g))
    pl.semaphore_wait(barrier, jnp.where(inner, 1, len(steps) * rows - 1))

    def remote(src, dst, s, t, row, expert):
        return pltpu.make_async_remote_copy(src_ref=src, dst_ref=dst, send_sem=s, recv_sem=t,
                                            device_id={"row": row, "expert": expert}, device_id_type=MESH)

    cuts = [(0, height)]
    if height % LANES == 0 and height > LANES:
        top = max(1, 3 * height // LANES // 4) * LANES
        cuts = [(0, top), (top, height - top)]

    def cut(i):
        if len(cuts) == 1:
            return piece(mirror, lead)
        off, size = cuts[i]
        c = r ^ mirror
        src = base.at[lead, pl.ds(off, size), pl.ds(pl.multiple_of(c * width, width), width)]
        return remote(src, got.at[lead, r, pl.ds(off, size)], tsend.at[i], trecv.at[i], c, to[lead])

    def piece(m, j):
        c = r ^ m
        columns = pl.ds(pl.multiple_of(c * width, width), width)
        src = base.at[j, :, columns] if j == lead else held.at[:, columns]
        if dist[j] == 0 and isinstance(m, int) and m == 0:
            return pltpu.make_async_copy(src, got.at[j, r], recv.at[j, 0])
        return remote(src, got.at[j, r], send.at[j, m], recv.at[j, m], c, to[j])

    leads = [m for m in order if m >= half]

    def send_lead(m):
        if m < half:
            piece(m, lead).start()
            return
        q = leads.index(m)

        @pl.when(inner)
        def _():
            piece(leads[q - 1], lead).start()

        @pl.when(jnp.logical_not(inner))
        def _():
            if m == mirror:
                for i in range(len(cuts)):
                    cut(i).start()
            else:
                piece(m, lead).start()

    unit = unit_of(height)
    span = unit * height
    loads = [
        pltpu.make_async_copy(base.at[other], held, near.at[0]),
        pltpu.make_async_copy(right.at[other], right_all.at[r], near.at[1]),
        pltpu.make_async_copy(left.at[other, :, pl.ds(pl.multiple_of(r // unit * span, LANES), span)],
                              left_own.at[r], near.at[2]),
        pltpu.make_async_copy(scale, scale_own, near.at[3]),
    ]
    for copy in loads:
        copy.start()

    @pl.when(inner)
    def _():
        cut(0).start()
        pl.semaphore_wait(go, 1)

    @pl.when(jnp.logical_not(inner))
    def _():
        pl.semaphore_signal(go, inc=1, device_id={"row": r ^ quarter, "expert": g}, device_id_type=MESH)

    first = []
    for src, dst, s, t in (
        (left.at[lead], left_all.at[r], lsend.at[0], lrecv.at[0]),
        (right.at[lead], right_got, ssend.at[0], srecv.at[0]),
        (scale, scale_got, ssend.at[1], srecv.at[1]),
    ):
        if dist[lead] == 0:
            copy = pltpu.make_async_copy(src, dst, t)
        else:
            copy = remote(src, dst, s, t, r, to[lead])
        first.append(copy)
    first.append(remote(left.at[lead], left_all.at[r], lsend.at[half], lrecv.at[half], r ^ half, to[lead]))
    for m in (*range(half, rows), *range(1, half)):
        c = r ^ m
        part = left.at[other, :, pl.ds(pl.multiple_of(c // unit * span, LANES), span)]
        first.append(remote(part, left_own.at[r], asend.at[m], arecv.at[m], c, g))
    for m in (half, *range(1, half)):
        first.append(remote(right.at[other], right_all.at[r], rsend.at[0, m], rrecv.at[0, m], r ^ m, g))
    for copy in first:
        copy.start()

    pl.when(jnp.logical_not(inner))(piece(order[0], lead).start)

    def right_round():
        part = right_all.at[r ^ half]
        copies = [remote(part, part, rsend.at[1, m], rrecv.at[1, m], r ^ m, g) for m in range(1, half)]
        for copy in copies:
            copy.start()
        return copies

    def left_round(mask, have):
        copies = []
        for s in have:
            part = left_all.at[r ^ s]
            copy = remote(part, part, lsend.at[mask | s], lrecv.at[mask | s], r ^ mask, g)
            copy.start()
            copies.append(copy)
        return copies

    rounds = []
    mask, have = half // 2, [0, half]
    while mask:
        rounds.append((mask, list(have)))
        have += [s | mask for s in have]
        mask //= 2

    early = len(order) if dist[lead] == 0 else len(order) // 4
    for m in order[1:early]:
        send_lead(m)
    ahead = [first[3], first[3 + rows]]
    first[0].wait()
    for copy in ahead:
        copy.wait_recv()
    waiting = right_round() + left_round(*rounds[0])
    for m in order[early:]:
        send_lead(m)
    for copy in ahead:
        copy.wait_send()
    for copy in first[1:3] + first[4:3 + rows] + first[4 + rows:] + waiting + loads:
        copy.wait()
    waiting = left_round(*rounds[1])

    def expand(lhs, rhs):
        return lax.dot_general(lhs, rhs, (((0,), (0,)), ((), ())), preferred_element_type=jnp.float32)

    rank_all = left_all.shape[0] * left_all.shape[1]

    def merge_held(q, carry):
        c = r ^ q ^ half
        delta = expand(left_own[...].reshape(rank_all, span), right_all[c])
        part = delta[:height]
        for u in range(1, unit):
            part = jnp.where(lax.rem(r, unit) == u, delta[u * height:(u + 1) * height], part)
        here = pl.ds(pl.multiple_of(c * width, width), width)
        held[:, here] = (held[:, here].astype(jnp.float32) + scale_own[other] * part).astype(held.dtype)
        return carry

    lax.fori_loop(0, rows, merge_held, 0)
    far, close = order[::2], order[1::2]
    bunch = len(far) if dist[lead] == 0 else len(far) // 2
    for i in range(0, len(far), bunch):
        for m in far[i:i + bunch] + close[i:i + bunch]:
            piece(m, other).start()
    for i in range(1, len(cuts)):
        pl.when(inner)(cut(i).start)
    for copy in waiting:
        copy.wait()
    for i in range(2, len(rounds)):
        for copy in left_round(*rounds[i]):
            copy.wait()

    def merge(row, off, size):
        columns = pl.ds(pl.multiple_of(row * height + off, LANES), size)
        return expand(left_all[:, :, columns].reshape(rank_all, size), right_got[...])

    blocks = rows // unit
    calm = blocks - blocks // 4

    def turn(q, carry):
        m = jnp.where(q < calm, q, calm + blocks - 1 - q) * unit
        row = (r ^ m) // unit * unit
        for u in range(unit):
            block = got.at[lead, r ^ (m + u)]
            remote(block, block, send.at[lead, m + u], recv.at[lead, m + u], r ^ 1, g).wait_recv()
        delta = merge(row, 0, span)
        for u in range(unit):
            part = delta[u * height:(u + 1) * height]
            got[lead, row + u] = (got[lead, row + u].astype(jnp.float32) + scale_got[lead] * part).astype(got.dtype)
        return carry

    lax.fori_loop(0, blocks - (len(cuts) > 1), turn, 0)
    for m in order:
        piece(m, other).wait_recv()
    row = r ^ mirror
    for i, (off, size) in enumerate(cuts if len(cuts) > 1 else ()):
        cut(i).wait_recv()
        here = pl.ds(off, size)
        part = scale_got[lead] * merge(row, off, size)
        got[lead, row, here] = (got[lead, row, here].astype(jnp.float32) + part).astype(got.dtype)
    for m in order:
        piece(m, other).wait_send()
        if m == mirror:
            for i in range(len(cuts)):
                cut(i).wait_send()
        elif m or dist[lead]:
            piece(m, lead).wait_send()


def exchange(first, groups, rows, base, left, right, scale):
    dist = (first, groups - 1 - first)
    slots, height, total = base.shape
    width = total // rows
    rank, model = left.shape[1:]
    anywhere = pl.BlockSpec(memory_space=pl.ANY)
    dma = pltpu.SemaphoreType.DMA
    served = pl.pallas_call(
        functools.partial(exchange_kernel, dist, groups, rows),
        out_shape=jax.ShapeDtypeStruct((slots, rows, height, width), base.dtype),
        in_specs=[anywhere] * 4,
        out_specs=pl.BlockSpec(memory_space=pltpu.VMEM),
        scratch_shapes=[
            pltpu.VMEM((rows, rank, model), left.dtype),
            pltpu.VMEM(right.shape[1:], right.dtype),
            pltpu.SMEM(scale.shape, scale.dtype),
            pltpu.VMEM((height, total), base.dtype),
            pltpu.VMEM((rows, rank, unit_of(height) * height), left.dtype),
            pltpu.VMEM((rows, *right.shape[1:]), right.dtype),
            pltpu.SMEM(scale.shape, scale.dtype),
            dma((slots, rows)), dma((slots, rows)),
            dma((2,)), dma((2,)),
            dma((rows,)), dma((rows,)),
            dma((2,)), dma((2,)),
            pltpu.SemaphoreType.REGULAR,
            dma((rows,)), dma((rows,)),
            dma((2, rows)), dma((2, rows)),
            dma((4,)),
        ],
        compiler_params=pltpu.CompilerParams(collective_id=first, has_side_effects=True, vmem_limit_bytes=VMEM_LIMIT),
        name=f"exchange_{first}",
    )(base, left, right, scale)
    return copy_out(served.reshape(slots, rows * height, width))


def copy_out_kernel(chunks, x, y, sem):
    size = x.shape[1] // chunks
    copies = []
    for j in range(x.shape[0]):
        for i in range(chunks):
            here = pl.ds(i * size, size)
            copies.append(pltpu.make_async_copy(x.at[j, here], y.at[j, here], sem.at[j, i]))
    for copy in copies:
        copy.start()
    for copy in copies:
        copy.wait()


def copy_out(x, chunks=7):
    return pl.pallas_call(
        functools.partial(copy_out_kernel, chunks),
        out_shape=pltpu.HBM(x.shape, x.dtype),
        in_specs=[pl.BlockSpec(memory_space=pltpu.VMEM)],
        out_specs=pl.BlockSpec(memory_space=pl.ANY),
        scratch_shapes=[pltpu.SemaphoreType.DMA((x.shape[0], chunks))],
        compiler_params=pltpu.CompilerParams(vmem_limit_bytes=VMEM_LIMIT),
        name="copy_out",
    )(x)


def local(groups, rows, base, left_factors, right_factors, expert_adapter_scale, placement):
    first = jnp.mod(placement[0] - lax.axis_index("expert"), groups)
    left = jnp.swapaxes(left_factors, 1, 2)
    served = lax.switch(
        first,
        [functools.partial(exchange, o, groups, rows) for o in range(groups)],
        base, left, right_factors, expert_adapter_scale,
    )
    return served


def solution(mesh):
    placed = (
        P("expert", "row", None),
        P("expert", None, "row"),
        P("expert", None, "row"),
        P("expert"),
        P("expert"),
    )
    return jax.shard_map(
        functools.partial(local, mesh.shape["expert"], mesh.shape["row"]),
        mesh=mesh, in_specs=placed, out_specs=P("expert", None, "row"), check_vma=False,
    )
```
